32 devices in a mesh: seq: 4 (over y, x), exp: 8 (over z, core).
Axes of the slice: x: 2, y: 2, z: 4, core: 2. Of those that a mesh axis runs over, the one named last changes fastest.
Arguments:
- gates: float32 [4096, 2], P(('seq', 'exp')), may hold values from 0.1 to 0.9
- expert_ids: int32 [4096, 2], P(('seq', 'exp')), may hold values from 0 to 7, all different within a row; in each aligned block of 128 rows (0 to 127, 128 to 255, ...) at most 32 rows name the same one
- saved_pre: bfloat16 [8, 1024, 2, 7168], P('exp', None, None, 'seq'), may hold values from -6 to 6
- w_down: bfloat16 [8, 7168, 4096], P('exp', 'seq'), may hold values from -0.0625 to 0.0625
- residual_grad: bfloat16 [4096, 4096], P(('seq', 'exp')), may hold values from -6 to 6
- in_weight: bfloat16 [4096, 2048], P('seq', 'exp'), may hold values from -0.125 to 0.125
- ssm_in: bfloat16 [4096, 2048], P('seq', 'exp'), may hold values from -0.59765625 to 0.59765625
- b_proj: bfloat16 [4096, 128], P('seq'), may hold values from -0.546875 to 0.546875
- c_proj: bfloat16 [4096, 128], P('seq'), may hold values from -0.546875 to 0.546875
- step_sizes: float32 [32, 4096], P('exp', 'seq'), may hold values from 0.05 to 1149.88
- a_log: float32 [32], P('exp'), may hold values from -12 to 0
- skip_gain: float32 [32], P('exp'), may hold values from 0.5 to 1.5
- ssm_grad: bfloat16 [4096, 2048], P('seq', 'exp'), may hold values from -6 to 6
Outputs:
- pre_grads: bfloat16 [8, 1024, 2, 7168], P('exp', None, None, 'seq')
- route_grads: float32 [4096, 2], P(('seq', 'exp'))
- b_grads: float32 [4096, 128], P(('seq', 'exp'))
- c_grads: float32 [4096, 128], P(('seq', 'exp'))
- step_grads: float32 [32, 4096], P('exp', 'seq')
The draws below stay inside these ranges and needn't reach their ends.
Inputs may be any that keep to these rules, and one draw needn't show every extreme that they name: `expert_ids`: in each aligned block of 128 rows every expert is named by exactly 32 entries, and a row names 2 different experts.
All inputs are finite; a program needn't handle non-finite values.
Results may differ from the reference program's by a relative error of at most 0.019.
Values may be sent and summed in bfloat16 or wider, within the bound.
A program may use at most 192 MiB of HBM per device.

```python
import math
import jax
import jax.numpy as jnp
import numpy as np
from jax import lax

D = 4096
FFW = 7168
EXPERTS = 8
TOPK = 2
TOK_DEV = 128
TIME_HORIZON = 4096
TOKENS = 4096
CAP = 32
ESLOTS = 1024
HEAD_DEV = 4
CHANNEL_GROUPS = 32
HDIM = 64
NSTATE = 128
SPAN = 256
N_SEQ = 4
N_EXP = 8


def rate_fields(key):
    sampler_seeds = jax.random.split(jax.random.fold_in(key, 11), 6)
    fast_share = 0.5
    fast_heads = jax.random.uniform(sampler_seeds[0], (CHANNEL_GROUPS,)) < fast_share
    fast_rate = jax.random.uniform(sampler_seeds[1], (CHANNEL_GROUPS,), minval=0.2, maxval=0.35)
    slow_rate = jnp.exp(jax.random.uniform(sampler_seeds[2], (CHANNEL_GROUPS,), minval=jnp.log(0.2), maxval=jnp.log(0.6))) / (0.11 * TIME_HORIZON)
    forgetting_multiplier = jnp.where(fast_heads, fast_rate, slow_rate)
    drawn_increments = jnp.exp(jax.random.uniform(sampler_seeds[3], (CHANNEL_GROUPS, TIME_HORIZON), minval=jnp.log(0.05), maxval=jnp.log(0.2)))
    surge_instant = jax.random.randint(sampler_seeds[4], (3,), 0, TIME_HORIZON)
    surge_indicator = jnp.any(jnp.arange(TIME_HORIZON)[None, :] == surge_instant[:, None], axis=0)
    surge_magnitude = jax.random.uniform(sampler_seeds[5], (CHANNEL_GROUPS, TIME_HORIZON), minval=0.22, maxval=0.5)
    increment_elements = jnp.where(surge_indicator[None, :], surge_magnitude / forgetting_multiplier[:, None], drawn_increments)
    return (jnp.log(forgetting_multiplier).astype(jnp.float32), increment_elements.astype(jnp.float32))


def draw_a_log(key, part):
    return rate_fields(key)[0]


def draw_step_sizes(key, part):
    return rate_fields(key)[1]


def block_scale(rng, shape, shards, smallest, top_value):
    gain, own = 1.0, jax.random.fold_in(rng, 6)
    for axis_at, shards_of in shards:
        draws = jnp.exp(jax.random.uniform(jax.random.fold_in(own, axis_at), (shards_of,), jnp.float32, smallest / len(shards), top_value / len(shards)))
        gain = gain * jnp.repeat(draws, shape[axis_at] // shards_of).reshape([-1 if axis == axis_at else 1 for axis in range(len(shape))])
    return gain


def deal_out(key, own, number, rows, count, top, bound, skew):
    order = jax.random.permutation(key, count)
    heavy_load, common = shares(count, rows * top, bound, skew, True), shares(count, rows * top, bound, skew, False)
    places = jnp.arange(count)

    def named(tallies, rotation):
        used = int((tallies > 0).sum())
        fixed = max(1, used // 4)
        shifted = fixed + (places - fixed + rotation * (used - fixed)) % max(1, count - fixed)
        return jnp.zeros((count,), jnp.int32).at[order[jnp.where(places < fixed, places, shifted)]].set(jnp.asarray(tallies, jnp.int32))

    tallies = jnp.where(number % 4 == 0, named(heavy_load, number // 4), named(common, number - number // 4 - 1))
    mixed = jax.random.permutation(jax.random.fold_in(own, 3), count)
    source_of, sink = mixed[0:count // 2 * 2:2], mixed[1:count // 2 * 2:2]
    room = jnp.minimum(tallies[source_of] - 1, bound - tallies[sink]) // 2
    room = jnp.where((source_of == order[0]) | (sink == order[0]) | (tallies[sink] == 0), 0, jnp.maximum(room, 0))
    shifted = jax.random.randint(jax.random.fold_in(own, 4), (count // 2,), 0, 1 << 20) % (room + 1)
    tallies = tallies.at[source_of].add(-shifted).at[sink].add(shifted)
    items = jnp.searchsorted(jnp.cumsum(tallies), jnp.arange(rows * top), side="right").astype(jnp.int32)
    table = items.reshape(top, rows).T
    table = table[jax.random.permutation(jax.random.fold_in(own, 1), rows)]
    rotation = jax.random.randint(jax.random.fold_in(own, 2), (rows, 1), 0, top)
    return jnp.take_along_axis(table, (jnp.arange(top)[None, :] + rotation) % top, axis=1)


def shares(number_of, total, bound, lean, full):
    weights = [(1 << 20) // math.isqrt(standing ** lean) + 1 for standing in range(1, number_of + 1)]
    largest = bound if full else min(bound, max(-(-total // number_of), total * weights[0] // sum(weights)))
    least = 1 if total - largest >= number_of - 1 else 0
    counts, spare = [largest] + [least] * (number_of - 1), total - largest - least * (number_of - 1)
    while spare > 0:
        free = [i for i in range(1, number_of) if counts[i] < largest] or [i for i in range(1, number_of) if counts[i] < bound]
        whole, remaining = sum([weights[i] for i in free]), spare
        for i in free:
            addition = min(bound - counts[i], max(1, remaining * weights[i] // whole), spare)
            counts[i] = counts[i] + addition
            spare = spare - addition
    return np.array(counts)


def gaussian(stream_key, shape, scale, reach, cuts=(), kind=jnp.bfloat16):
    values = scale * jax.random.normal(stream_key, shape, jnp.float32)
    if cuts:
        values = values * block_scale(stream_key, shape, cuts, -0.22, 0.18)
    return jnp.clip(values, -reach, reach).astype(kind)


def setup_inputs(seed: int = 0) -> dict:
    seeds = jax.random.split(jax.random.key(seed), 14)
    gates = jnp.clip(0.1 + 0.79999997 * jax.random.uniform(seeds[0], (TOKENS, TOPK), jnp.float32) ** block_scale(seeds[0], (TOKENS, TOPK), ((0, 32),), -0.2, 0.2), 0.1, 0.9)
    expert_ids_keys = jax.random.split(jax.random.fold_in(seeds[1], 1), TOKENS // TOK_DEV)
    expert_ids_turns = jax.random.permutation(jax.random.fold_in(seeds[1], 3), TOKENS // TOK_DEV)
    expert_ids = jax.vmap(lambda own, number: deal_out(jax.random.fold_in(seeds[1], 2), own, number, TOK_DEV, EXPERTS, TOPK, CAP, 0))(expert_ids_keys, expert_ids_turns).reshape((TOKENS, TOPK))
    saved_pre = gaussian(seeds[2], (EXPERTS, ESLOTS, 2, FFW), 1.0, 6.0, ((0, 8), (3, 4)))
    w_down = gaussian(seeds[3], (EXPERTS, FFW, D), FFW ** -0.5, 0.0625, ((0, 8), (1, 4)))
    residual_grad = gaussian(seeds[4], (TOKENS, D), 1.0, 6.0, ((0, 32),))
    in_weight = gaussian(seeds[5], (D, CHANNEL_GROUPS * HDIM), (CHANNEL_GROUPS * HDIM) ** -0.5, 0.125, ((0, 4), (1, 8)))
    ssm_in = gaussian(seeds[6], (TIME_HORIZON, CHANNEL_GROUPS * HDIM), 0.1, 0.59765625, ((0, 4), (1, 8)))
    b_proj = gaussian(seeds[7], (TIME_HORIZON, NSTATE), 0.088, 0.546875, ((0, 4),))
    c_proj = gaussian(seeds[8], (TIME_HORIZON, NSTATE), 0.088, 0.546875, ((0, 4),))
    step_sizes = draw_step_sizes(jax.random.fold_in(seeds[13], 71), 0)
    a_log = draw_a_log(jax.random.fold_in(seeds[13], 71), 0)
    skip_gain = jnp.clip(0.5 + 1.0 * jax.random.uniform(seeds[11], (CHANNEL_GROUPS,), jnp.float32) ** block_scale(seeds[11], (CHANNEL_GROUPS,), ((0, 8),), -0.2, 0.2), 0.5, 1.5)
    ssm_grad = gaussian(seeds[12], (TIME_HORIZON, CHANNEL_GROUPS * HDIM), 1.0, 6.0, ((0, 4), (1, 8)))
    return dict(gates=gates, expert_ids=expert_ids, saved_pre=saved_pre, w_down=w_down, residual_grad=residual_grad, in_weight=in_weight, ssm_in=ssm_in, b_proj=b_proj, c_proj=c_proj, step_sizes=step_sizes, a_log=a_log, skip_gain=skip_gain, ssm_grad=ssm_grad)


PRECISE = lax.Precision.HIGHEST

def span_scan(heads_input, b_values, c_values, log_decay, skip_values, start_state):
    head_count, length, head_size = heads_input.shape
    state_size = b_values.shape[1]
    blocks = length // SPAN
    x_spans = heads_input.reshape(head_count, blocks, SPAN, head_size).transpose(1, 0, 2, 3)
    b_spans = b_values.reshape(blocks, SPAN, state_size)
    c_spans = c_values.reshape(blocks, SPAN, state_size)
    g_spans = log_decay.reshape(head_count, blocks, SPAN).transpose(1, 0, 2)
    lower_mask = jnp.tril(jnp.ones((SPAN, SPAN), jnp.bool_))

    def advance(carried_state, inputs):
        x_block, b_block, c_block, g_block = inputs
        cumulative = jnp.cumsum(g_block, axis=1)
        spread = cumulative[:, :, None] - cumulative[:, None, :]
        weights = jnp.where(lower_mask, jnp.exp(-jnp.where(lower_mask, spread, 0.0)), 0.0)
        scores = jnp.dot(c_block, b_block.T, precision=PRECISE)
        within = jnp.einsum('hij,ij,hjp->hip', weights, scores, x_block, precision=PRECISE)
        carried = jnp.einsum('hi,in,hpn->hip', jnp.exp(-cumulative), c_block, carried_state, precision=PRECISE)
        tail_decay = jnp.exp(cumulative - cumulative[:, -1:])
        fresh_state = jnp.einsum('hj,hjp,jn->hpn', tail_decay, x_block, b_block, precision=PRECISE)
        next_state = jnp.exp(-cumulative[:, -1])[:, None, None] * carried_state + fresh_state
        return (next_state, within + carried)
    final_state, outputs = lax.scan(advance, start_state, (x_spans, b_spans, c_spans, g_spans))
    output = outputs.transpose(1, 0, 2, 3).reshape(head_count, length, head_size)
    return (output + skip_values[:, None, None] * heads_input, final_state)

def swiglu_grads(upstream, gate_values, saved_rows):
    gate_pre = saved_rows[:, 0, :].astype(jnp.float32)
    up_pre = saved_rows[:, 1, :].astype(jnp.float32)
    sigmoid_gate = jax.nn.sigmoid(gate_pre)
    activated = gate_pre * sigmoid_gate
    route_part = lax.optimization_barrier(jnp.sum(activated * up_pre * upstream, axis=1))
    hidden_grad = gate_values[:, None] * upstream
    gate_grad = hidden_grad * up_pre * sigmoid_gate * (1.0 + gate_pre * (1.0 - sigmoid_gate))
    up_grad = hidden_grad * activated
    return (jnp.stack([gate_grad, up_grad], axis=1).astype(jnp.bfloat16), route_part)

def reference(gates, expert_ids, saved_pre, w_down, residual_grad, in_weight, ssm_in, b_proj, c_proj, step_sizes, a_log, skip_gain, ssm_grad):
    heads_input = ssm_in.astype(jnp.float32).reshape(TIME_HORIZON, CHANNEL_GROUPS, HDIM).transpose(1, 0, 2)
    grads_heads = ssm_grad.astype(jnp.float32).reshape(TIME_HORIZON, CHANNEL_GROUPS, HDIM).transpose(1, 0, 2)
    decay_rates = jnp.exp(a_log)

    def forward(inputs, b_values, c_values, sizes):
        outputs, unused = span_scan(inputs, b_values, c_values, sizes * decay_rates[:, None], skip_gain, jnp.zeros((CHANNEL_GROUPS, HDIM, NSTATE), jnp.float32))
        return outputs
    unused, pullback = jax.vjp(forward, heads_input, b_proj.astype(jnp.float32), c_proj.astype(jnp.float32), step_sizes)
    input_heads, b_grads, c_grads, step_grads = pullback(grads_heads)
    x_grad = input_heads.transpose(1, 0, 2).reshape(TIME_HORIZON, CHANNEL_GROUPS * HDIM).astype(jnp.bfloat16)
    group_width = HEAD_DEV * HDIM
    grad_groups = x_grad.reshape(TIME_HORIZON, N_EXP, group_width).transpose(1, 0, 2)
    weight_groups = in_weight.reshape(D, N_EXP, group_width).transpose(1, 0, 2)

    def add_group(total, pair):
        head_part = jnp.dot(pair[0], pair[1].T, preferred_element_type=jnp.float32).astype(jnp.bfloat16)
        head_part = lax.optimization_barrier(head_part).astype(jnp.float32)
        return (total + head_part, None)
    summed, unused_out = lax.scan(add_group, residual_grad.astype(jnp.float32), (grad_groups, weight_groups))
    moe_grad = summed.astype(jnp.bfloat16)
    device_count = N_SEQ * N_EXP
    per_block = expert_ids.reshape(device_count, TOK_DEV * TOPK)
    onehot = (per_block[:, :, None] == jnp.arange(EXPERTS, dtype=jnp.int32)[None, None, :]).astype(jnp.int32)
    running = jnp.cumsum(onehot, axis=1)
    position = lax.optimization_barrier(jnp.sum(onehot * running, axis=2)) - 1
    slot_row = (jnp.arange(device_count, dtype=jnp.int32)[:, None] * CAP + position).reshape(-1).astype(jnp.int32)
    expert_flat = per_block.reshape(-1).astype(jnp.int32)
    assignment = jnp.arange(TOKENS * TOPK, dtype=jnp.int32)
    table = jnp.zeros((EXPERTS, ESLOTS), jnp.int32).at[expert_flat, slot_row].set(assignment)
    gate_flat = gates.reshape(-1)

    def one_expert(expert_index):
        members = table[expert_index]
        row_block = moe_grad[members // TOPK]
        upstream = jnp.dot(row_block, w_down[expert_index].T, preferred_element_type=jnp.float32)
        return swiglu_grads(upstream, gate_flat[members], saved_pre[expert_index])
    pre_grads, route_slots = lax.map(one_expert, jnp.arange(EXPERTS, dtype=jnp.int32))
    route_grads = route_slots[expert_flat, slot_row].reshape(TOKENS, TOPK)
    return (pre_grads, route_grads, b_grads, c_grads, step_grads)
```

```python
import functools

import jax
import jax.numpy as jnp
from jax import lax
from jax.sharding import PartitionSpec as P
from jax.experimental import pallas as pl
from jax.experimental.pallas import tpu as pltpu

TOPK = 2
HDIM = 64
SPAN = 256


PRECISE = lax.Precision.HIGHEST
F32 = jnp.float32
BF16 = jnp.bfloat16


def mm(spec, a, b):
    return jnp.einsum(spec, a.astype(BF16), b.astype(BF16), preferred_element_type=F32)


def slot_positions(flat_ids, expert_count):
    entries = flat_ids.shape[1]
    onehot = (flat_ids[:, :, None] == jnp.arange(expert_count, dtype=jnp.int32)).astype(BF16)
    lower = jnp.tril(jnp.ones((entries, entries), BF16))
    running = jnp.einsum("ij,bje->bie", lower, onehot, preferred_element_type=F32)
    return jnp.sum(onehot.astype(F32) * running, axis=2).astype(jnp.int32) - 1


def ssm_part(ssm_in, b_proj, c_proj, step_sizes, a_log, skip_gain, ssm_grad):
    length, columns = ssm_in.shape
    heads = columns // HDIM
    state = b_proj.shape[1]
    blocks = length // SPAN
    parts = lax.axis_size("seq")
    me = lax.axis_index("seq")
    x = ssm_in.reshape(blocks, SPAN, heads, HDIM).transpose(2, 0, 1, 3)
    g = ssm_grad.reshape(blocks, SPAN, heads, HDIM).transpose(2, 0, 1, 3)
    b = b_proj.reshape(blocks, SPAN, state)
    c = c_proj.reshape(blocks, SPAN, state)
    rates = jnp.exp(a_log)
    q = (step_sizes * rates[:, None]).reshape(heads, blocks, SPAN)
    upper = jnp.triu(jnp.ones((SPAN, SPAN), F32))
    cum = jnp.einsum("hkj,ji->hki", q, upper, precision=PRECISE)
    total = cum[:, :, -1]
    head_decay = jnp.exp(-cum)
    tail_decay = jnp.exp(cum - total[:, :, None])
    block_decay = jnp.exp(-total)
    fresh = mm("hkjp,kjn->hkpn", tail_decay[..., None] * x.astype(F32), b)
    back = mm("hkjp,kjn->hkpn", head_decay[..., None] * g.astype(F32), c)
    end_state = fresh[:, 0]
    for k in range(1, blocks):
        end_state = block_decay[:, k, None, None] * end_state + fresh[:, k]
    entry_grad = back[:, blocks - 1]
    for k in range(blocks - 2, -1, -1):
        entry_grad = block_decay[:, k, None, None] * entry_grad + back[:, k]
    shard_decay = jnp.exp(-jnp.sum(total, axis=1))
    packed = jnp.concatenate(
        [
            end_state,
            entry_grad,
            jnp.broadcast_to(shard_decay[:, None, None], (heads, 16, state)),
        ],
        axis=1,
    ).astype(BF16)
    everyone = lax.all_gather(packed, "seq", axis=0).astype(F32)

    lower_mask = jnp.tril(jnp.ones((SPAN, SPAN), jnp.bool_))
    spread = cum[:, :, :, None] - cum[:, :, None, :]
    weights = jnp.where(lower_mask, jnp.exp(-jnp.where(lower_mask, spread, 0.0)), 0.0)
    scores = mm("kin,kjn->kij", c, b)
    pair = mm("hkip,hkjp->hkij", g, x)
    mixed = weights * scores[None]
    cross = weights * pair
    products = mixed * pair
    row_sum = jnp.sum(products, axis=3)
    column_sum = jnp.sum(products, axis=2)
    x_within = mm("hkij,hkip->hkjp", mixed, g)
    cross_sum = jnp.sum(cross, axis=0)
    b_within = mm("kij,kin->kjn", cross_sum, c)
    c_within = mm("kij,kjn->kin", cross_sum, b)

    entry = jnp.zeros((heads, HDIM, state), F32)
    leave = jnp.zeros((heads, HDIM, state), F32)
    for i in range(parts - 1):
        decay = everyone[i][:, 2 * HDIM : 2 * HDIM + 1, :]
        entry = jnp.where(i < me, decay * entry + everyone[i][:, :HDIM], entry)
    for i in range(parts - 1, 0, -1):
        decay = everyone[i][:, 2 * HDIM : 2 * HDIM + 1, :]
        leave = jnp.where(i > me, decay * leave + everyone[i][:, HDIM : 2 * HDIM], leave)
    entries = [entry]
    for k in range(blocks - 1):
        entries.append(block_decay[:, k, None, None] * entries[-1] + fresh[:, k])
    leaves = [leave]
    for k in range(blocks - 1, 0, -1):
        leaves.append(block_decay[:, k, None, None] * leaves[-1] + back[:, k])
    entries = jnp.stack(entries, axis=1)
    leaves = jnp.stack(leaves[::-1], axis=1)

    from_leave = tail_decay[..., None] * mm("kjn,hkpn->hkjp", b, leaves)
    from_entry = head_decay[..., None] * mm("kin,hkpn->hkip", c, entries)
    x_grad = x_within + from_leave + skip_gain[:, None, None, None] * g.astype(F32)
    x_grad = x_grad.transpose(1, 2, 0, 3).reshape(length, columns).astype(BF16)
    b_grad = b_within + mm("hkjp,hkpn->kjn", tail_decay[..., None] * x.astype(F32), leaves)
    c_grad = c_within + mm("hkip,hkpn->kin", head_decay[..., None] * g.astype(F32), entries)
    carried = jnp.sum(g.astype(F32) * from_entry, axis=3)
    leaving = jnp.sum(x.astype(F32) * from_leave, axis=3)
    through = block_decay * jnp.sum(leaves * entries, axis=(2, 3))
    after = jnp.einsum("hki,ij->hkj", row_sum - column_sum + carried, jnp.tril(jnp.ones((SPAN, SPAN), F32)), precision=PRECISE)
    before = jnp.einsum("hkj,ji->hki", leaving, jnp.triu(jnp.ones((SPAN, SPAN), F32), 1), precision=PRECISE)
    decay_grad = -(after + before + through[:, :, None])
    step_grads = decay_grad.reshape(heads, length) * rates[:, None]
    return (x_grad, b_grad.reshape(length, state), c_grad.reshape(length, state), step_grads)


MESH_IDS = pl.DeviceIdType.MESH
TRANSPOSED = (((1,), (1,)), ((), ()))


def col_tile(width):
    return 256 if width % 256 == 0 else 128


def expert_kernel(
    parts,
    groups,
    x_grad,
    entries,
    weight_in,
    outgoing,
    down_in,
    saved_in,
    out,
    totals_out,
    table,
    gates,
    picked,
    rows_all,
    weight,
    residual,
    down,
    moe,
    upstream,
    saved,
    staged,
    partial,
    route,
    route_in,
    totals,
    local_sem,
    saved_sem,
    staged_sem,
    send_sem,
    recv_sem,
    table_send,
    table_recv,
    pick_send,
    pick_recv,
    residual_send,
    residual_recv,
    route_sem,
):
    slots, columns = picked.shape[1:]
    capacity = slots // groups
    tokens = entries.shape[1]
    devices = parts * groups
    depth = weight.shape[0]
    hidden = down.shape[0]
    half = slots // 2
    me = lax.axis_index("seq")
    expert = lax.axis_index("exp")
    square = parts == 4
    peers = [lax.rem(me + o, parts) for o in range(1, parts)]
    beside = me + 1 - 2 * lax.rem(me, 2)
    across = lax.rem(me + 2, parts)
    corner = parts - 1 - me

    def local(source, target, number):
        return pltpu.make_async_copy(source, target, local_sem.at[number])

    weights_in = [
        local(weight_in.at[j], weight.at[:, pl.ds(j * columns, columns)], j)
        for j in range(groups)
    ]
    down_copy = local(down_in.at[0], down, groups)
    flat = me * groups + expert
    my_columns = pl.ds(pl.multiple_of(expert * columns, columns), columns)
    my_block = pl.ds(pl.multiple_of(flat * capacity, capacity), capacity)

    def outgoing_block(part, number):
        return outgoing.at[
            pl.ds(pl.multiple_of(number * capacity, capacity), capacity),
            pl.ds(pl.multiple_of(part * depth, depth), depth),
        ]

    own_entries = pltpu.make_async_copy(entries, table.at[flat], table_recv)
    own_rows = pltpu.make_async_copy(picked.at[expert], rows_all.at[me, :, my_columns], pick_recv)
    own_residual = pltpu.make_async_copy(
        outgoing_block(me, expert), residual.at[my_block], residual_recv.at[me]
    )

    def saved_copy(k):
        return pltpu.make_async_copy(
            saved_in.at[0, pl.ds(k * slots, slots)], saved.at[k % 2], saved_sem.at[k % 2]
        )

    def staged_copy(k):
        return pltpu.make_async_copy(
            staged.at[k % 2], out.at[0, pl.ds(k * slots, slots)], staged_sem.at[k % 2]
        )

    own_entries.start()
    own_residual.start()
    for copy in weights_in:
        copy.start()
    saved_copy(0).start()
    down_copy.start()

    barrier = pltpu.get_barrier_semaphore()

    def device(other):
        return (lax.div(other, groups), lax.rem(other, groups))

    def greet(o, carry):
        other = lax.rem(flat + o, devices)
        pl.semaphore_signal(barrier, inc=1, device_id=device(other), device_id_type=MESH_IDS)
        return carry

    lax.fori_loop(1, devices, greet, 0)
    pl.semaphore_wait(barrier, devices - 1)

    def pick_copy(o):
        other = lax.rem(expert + o, groups)
        return pltpu.make_async_remote_copy(
            src_ref=picked.at[other],
            dst_ref=rows_all.at[me, :, my_columns],
            send_sem=pick_send,
            recv_sem=pick_recv,
            device_id=(me, other),
            device_id_type=MESH_IDS,
        )

    def residual_copy(o):
        other = lax.rem(flat + o, devices)
        return pltpu.make_async_remote_copy(
            src_ref=outgoing_block(*device(other)),
            dst_ref=residual.at[my_block],
            send_sem=residual_send,
            recv_sem=residual_recv.at[me],
            device_id=device(other),
            device_id_type=MESH_IDS,
        )

    def start_pick(o, carry):
        pick_copy(o).start()
        return carry

    def start_residual(o, carry):
        residual_copy(o).start()
        return carry

    def start_entries(o, carry):
        other = lax.rem(flat + o, devices)
        pltpu.make_async_remote_copy(
            src_ref=entries,
            dst_ref=table.at[flat],
            send_sem=table_send,
            recv_sem=table_recv,
            device_id=device(other),
            device_id_type=MESH_IDS,
        ).start()
        return carry

    def pick(b, carry):
        entry = table[me * groups + b]
        numbers = lax.broadcasted_iota(jnp.int32, (slots, tokens), 0).astype(F32)
        hit = jnp.zeros((slots, tokens), F32)
        for j in range(TOPK):
            hit = jnp.where(numbers == entry[j : j + 1], 1.0, hit)
        block = x_grad[pl.ds(pl.multiple_of(b * tokens, tokens), tokens), :]
        found = jnp.dot(hit.astype(BF16), block, preferred_element_type=F32).astype(BF16)
        place = pl.ds(pl.multiple_of(b * capacity, capacity), capacity)
        picked[:, place, :] = found.reshape(groups, capacity, columns)
        return carry

    def gate(block, carry):
        entry = table[block]
        numbers = lax.broadcasted_iota(jnp.int32, (capacity, tokens), 0) + expert * capacity
        numbers = numbers.astype(F32)
        value = jnp.zeros((capacity, tokens), F32)
        for j in range(TOPK):
            value = jnp.where(numbers == entry[j : j + 1], entry[TOPK + j : TOPK + j + 1], value)
        place = pl.ds(pl.multiple_of(block * capacity, capacity), capacity)
        gates[place, :] = jnp.sum(value, axis=1, keepdims=True)
        return carry

    def await_all(block, sem):
        pltpu.make_async_copy(block, block, sem).wait()

    def piece(phase, owner, number):
        span = slots if number is None else half
        first = 0 if number is None else number * half
        if phase == 0:
            return rows_all.at[owner, pl.ds(first, span)]
        start = pl.multiple_of(owner * depth, depth)
        return moe.at[phase - 1, pl.ds(first, span), pl.ds(start, depth)]

    def remote(phase, owner, number, peer, index):
        block = piece(phase, owner, number)
        return pltpu.make_async_remote_copy(
            src_ref=block,
            dst_ref=block,
            send_sem=send_sem.at[phase, index],
            recv_sem=recv_sem.at[phase, index],
            device_id=(peer, expert),
            device_id_type=MESH_IDS,
        )

    def sends(phase):
        if not square:
            return [remote(phase, me, None, peers[o], o) for o in range(parts - 1)]
        return [
            remote(phase, me, 1, beside, 1),
            remote(phase, me, 0, across, 2),
            remote(phase, me, 0, beside, 0),
            remote(phase, me, 1, across, 3),
        ]

    def forward_across(phase):
        return remote(phase, beside, 1, across, 5)

    def forward_beside(phase):
        return remote(phase, across, 0, beside, 4)

    def start(phase):
        for copy in sends(phase):
            copy.start()

    def relay(phase):
        if square:
            remote(phase, beside, 1, beside, 1).wait_recv()
            forward_across(phase).start()
            remote(phase, across, 0, across, 2).wait_recv()
            forward_beside(phase).start()

    def arrive(phase):
        if square:
            remote(phase, beside, 0, beside, 0).wait_recv()
            remote(phase, across, 1, across, 3).wait_recv()
            remote(phase, corner, 0, beside, 4).wait_recv()
            remote(phase, corner, 1, across, 5).wait_recv()
        else:
            for o in range(parts - 1):
                owner = lax.rem(me + parts - 1 - o, parts)
                remote(phase, owner, None, peers[o], o).wait_recv()

    def finish(phase):
        for copy in sends(phase):
            copy.wait_send()
        if square:
            forward_across(phase).wait_send()
            forward_beside(phase).wait_send()

    def project(k):
        tile = col_tile(depth)
        rows = rows_all.at[k]
        await_all(residual.at[pl.ds(k * slots, slots)], residual_recv.at[k])

        def step(i, carry):
            first = pl.multiple_of(i * tile, tile)
            total = lax.dot_general(
                rows[...], weight[pl.ds(first, tile), :], TRANSPOSED,
                preferred_element_type=F32,
            )
            total = total + residual[pl.ds(k * slots, slots), pl.ds(first, tile)].astype(F32)
            place = pl.multiple_of(me * depth + first, tile)
            moe[k, :, pl.ds(place, tile)] = total.astype(BF16)
            return carry

        lax.fori_loop(0, depth // tile, step, 0)

    def expand(k):
        tile = col_tile(hidden)

        def step(i, carry):
            first = pl.multiple_of(i * tile, tile)
            upstream[:, pl.ds(first, tile)] = lax.dot_general(
                moe[k], down[pl.ds(first, tile), :], TRANSPOSED,
                preferred_element_type=F32,
            )
            return carry

        lax.fori_loop(0, hidden // tile, step, 0)

    def activate(k):
        tile = 32
        lanes = 128

        def step(i, carry):
            first = pl.multiple_of(i * tile, tile)
            rows = pl.ds(first, tile)
            gate_pre = saved[k % 2, rows, 0, :].astype(F32)
            up_pre = saved[k % 2, rows, 1, :].astype(F32)
            up = upstream[rows, :]
            sigmoid_gate = 1.0 / (1.0 + jnp.exp(-gate_pre))
            activated = gate_pre * sigmoid_gate
            product = activated * up_pre * up
            total = product[:, :lanes]
            for j in range(1, hidden // lanes):
                total = total + product[:, j * lanes : (j + 1) * lanes]
            partial[rows, :] = total
            scale = gates[pl.ds(pl.multiple_of(k * slots + first, tile), tile), :]
            hidden_grad = scale * up
            gate_grad = hidden_grad * up_pre * sigmoid_gate * (1.0 + gate_pre * (1.0 - sigmoid_gate))
            staged[k % 2, rows, 0, :] = gate_grad.astype(BF16)
            staged[k % 2, rows, 1, :] = (hidden_grad * activated).astype(BF16)
            return carry

        lax.fori_loop(0, slots // tile, step, 0)
        sums = jnp.sum(partial[...].T, axis=0, keepdims=True)
        route[k] = sums

        @pl.when(me == k)
        def _():
            route_in[k] = sums

        @pl.when(me != k)
        def _():
            route_copy(k).start()

    def route_copy(k):
        return pltpu.make_async_remote_copy(
            src_ref=route.at[k],
            dst_ref=route_in.at[me],
            send_sem=route_sem.at[0],
            recv_sem=route_sem.at[1],
            device_id=(k, expert),
            device_id_type=MESH_IDS,
        )

    def total_copy(o):
        return pltpu.make_async_remote_copy(
            src_ref=totals.at[expert],
            dst_ref=totals.at[expert],
            send_sem=route_sem.at[2],
            recv_sem=route_sem.at[3],
            device_id=(me, lax.rem(expert + o, groups)),
            device_id_type=MESH_IDS,
        )

    def send_totals():
        await_all(route_in.at[pl.ds(0, parts - 1)], route_sem.at[1])
        total = route_in[0]
        for k in range(1, parts):
            total = total + route_in[k]
        totals[expert] = total
        for o in range(1, groups):
            total_copy(o).start()

    def receive_totals():
        await_all(totals.at[pl.ds(0, groups - 1)], route_sem.at[3])
        totals_out[...] = totals[...]
        await_all(route.at[pl.ds(0, parts - 1)], route_sem.at[0])
        await_all(totals.at[pl.ds(0, groups - 1)], route_sem.at[2])

    lax.fori_loop(1, devices, start_entries, 0)
    await_all(table, table_recv)
    lax.fori_loop(0, groups, pick, 0)
    lax.fori_loop(0, devices, gate, 0)
    own_rows.start()
    lax.fori_loop(1, groups, start_pick, 0)
    lax.fori_loop(1, devices, start_residual, 0)
    await_all(rows_all.at[me], pick_recv)
    start(0)
    for copy in weights_in:
        copy.wait()
    relay(0)
    arrive(0)
    project(0)
    start(1)
    if parts > 1:
        project(1)
    relay(1)
    start(2)
    project(2)
    down_copy.wait()
    for k in range(parts):
        arrive(k + 1)
        if k + 1 < parts:
            saved_copy(k + 1).start()
        expand(k)
        if k + 1 < parts:
            relay(k + 2)
            if k + 2 < parts:
                start(k + 3)
                if k + 3 < parts:
                    project(k + 3)
        saved_copy(k).wait()
        if k >= 2:
            staged_copy(k - 2).wait()
        activate(k)
        staged_copy(k).start()
    send_totals()
    await_all(table.at[pl.ds(0, devices - 1)], table_send)
    await_all(picked.at[pl.ds(0, groups - 1)], pick_send)
    await_all(residual.at[pl.ds(0, (devices - 1) * capacity)], residual_send)
    for phase in range(parts + 1):
        finish(phase)
    receive_totals()
    for k in range(max(0, parts - 2), parts):
        staged_copy(k).wait()


def expert_part(x_grad, entries, weight, outgoing, w_down, saved_pre):
    groups = lax.axis_size("exp")
    parts = lax.axis_size("seq")
    slots = outgoing.shape[0]
    columns = x_grad.shape[1]
    depth = weight.shape[1]
    hidden = w_down.shape[1]
    width = w_down.shape[2]
    anywhere = pl.BlockSpec(memory_space=pl.ANY)
    in_vmem = pl.BlockSpec(memory_space=pltpu.VMEM)
    copies = 6 if parts == 4 else parts - 1
    return pl.pallas_call(
        functools.partial(expert_kernel, parts, groups),
        out_shape=(
            jax.ShapeDtypeStruct(saved_pre.shape, BF16),
            jax.ShapeDtypeStruct((groups, 1, slots), F32),
        ),
        in_specs=[in_vmem] * 2 + [anywhere] * 4,
        out_specs=(anywhere, in_vmem),
        scratch_shapes=[
            pltpu.VMEM((parts * groups, *entries.shape), F32),
            pltpu.VMEM((parts * slots, 1), F32),
            pltpu.VMEM((groups, slots, columns), BF16),
            pltpu.VMEM((parts, slots, groups * columns), BF16),
            pltpu.VMEM((depth, groups * columns), BF16),
            pltpu.VMEM((parts * slots, depth), BF16),
            pltpu.VMEM((hidden, width), BF16),
            pltpu.VMEM((parts, slots, width), BF16),
            pltpu.VMEM((slots, hidden), F32),
            pltpu.VMEM((2, slots, 2, hidden), BF16),
            pltpu.VMEM((2, slots, 2, hidden), BF16),
            pltpu.VMEM((slots, 128), F32),
            pltpu.VMEM((parts, 1, slots), F32),
            pltpu.VMEM((parts, 1, slots), F32),
            pltpu.VMEM((groups, 1, slots), F32),
            pltpu.SemaphoreType.DMA((groups + 1,)),
            pltpu.SemaphoreType.DMA((2,)),
            pltpu.SemaphoreType.DMA((2,)),
            pltpu.SemaphoreType.DMA((parts + 1, copies)),
            pltpu.SemaphoreType.DMA((parts + 1, copies)),
            pltpu.SemaphoreType.DMA,
            pltpu.SemaphoreType.DMA,
            pltpu.SemaphoreType.DMA,
            pltpu.SemaphoreType.DMA,
            pltpu.SemaphoreType.DMA,
            pltpu.SemaphoreType.DMA((parts,)),
            pltpu.SemaphoreType.DMA((4,)),
        ],
        compiler_params=pltpu.CompilerParams(
            collective_id=1, has_side_effects=True, vmem_limit_bytes=62 * 1024 * 1024
        ),
        cost_estimate=pl.CostEstimate(
            flops=2 * parts * slots * (width * hidden + groups * columns * depth),
            bytes_accessed=2 * (hidden * width + 4 * parts * slots * hidden),
            transcendentals=0,
        ),
    )(x_grad, entries, weight, outgoing, w_down, saved_pre)


def per_device(
    gates,
    expert_ids,
    saved_pre,
    w_down,
    residual_grad,
    in_weight,
    ssm_in,
    b_proj,
    c_proj,
    step_sizes,
    a_log,
    skip_gain,
    ssm_grad,
):
    expert_count = lax.axis_size("exp")
    parts = lax.axis_size("seq")
    my_expert = lax.axis_index("exp")
    tokens_here, width = residual_grad.shape
    per_block = tokens_here * TOPK
    capacity = per_block // expert_count
    slots = expert_count * capacity

    entry_ids = expert_ids.reshape(1, per_block)
    own_target = (entry_ids * capacity + slot_positions(entry_ids, expert_count)).reshape(
        tokens_here, TOPK
    )
    slot_numbers = jnp.arange(slots, dtype=jnp.int32)
    own_selector = jnp.any(own_target[None] == slot_numbers[:, None, None], axis=2).astype(BF16)
    outgoing = jnp.dot(own_selector, residual_grad, preferred_element_type=F32).astype(BF16)
    slice_weight = lax.all_gather(in_weight, "exp", axis=0)
    entries = jnp.concatenate([own_target.astype(F32).T, gates.T], axis=0)
    entries = jnp.pad(entries, ((0, -entries.shape[0] % 8), (0, 0)))
    x_grad, b_grad, c_grad, step_grads = ssm_part(
        ssm_in, b_proj, c_proj, step_sizes, a_log, skip_gain, ssm_grad
    )

    both = jnp.concatenate([b_grad, c_grad], axis=1)
    both, slice_weight = lax.optimization_barrier((both, slice_weight))
    pre_grad, totals = expert_part(
        x_grad, entries, slice_weight, outgoing, w_down, saved_pre
    )
    both = lax.psum_scatter(both, "exp", scatter_dimension=0, tiled=True)
    state = b_proj.shape[1]

    totals = lax.dynamic_slice_in_dim(totals[:, 0, :], my_expert * capacity, capacity, 1)
    totals = totals.reshape(-1)
    chosen = own_target.reshape(per_block, 1) == slot_numbers[None, :]
    route_grads = jnp.sum(jnp.where(chosen, totals[None, :], 0.0), axis=1)
    return (
        pre_grad,
        route_grads.reshape(tokens_here, TOPK),
        both[:, :state],
        both[:, state:],
        step_grads,
    )


def solution(mesh):
    in_specs = (
        P(("seq", "exp"), None),
        P(("seq", "exp"), None),
        P("exp", None, None, "seq"),
        P("exp", "seq", None),
        P(("seq", "exp"), None),
        P("seq", "exp"),
        P("seq", "exp"),
        P("seq", None),
        P("seq", None),
        P("exp", "seq"),
        P("exp"),
        P("exp"),
        P("seq", "exp"),
    )
    out_specs = (
        P("exp", None, None, "seq"),
        P(("seq", "exp"), None),
        P(("seq", "exp"), None),
        P(("seq", "exp"), None),
        P("exp", "seq"),
    )
    return jax.shard_map(
        per_device, mesh=mesh, in_specs=in_specs, out_specs=out_specs, check_vma=False
    )
```

```python
import functools

import jax
import jax.numpy as jnp
from jax import lax
from jax.sharding import PartitionSpec as P
from jax.experimental import pallas as pl
from jax.experimental.pallas import tpu as pltpu

TOPK = 2
HDIM = 64
SPAN = 256


PRECISE = lax.Precision.HIGHEST
F32 = jnp.float32
BF16 = jnp.bfloat16


def mm(spec, a, b):
    return jnp.einsum(spec, a.astype(BF16), b.astype(BF16), preferred_element_type=F32)


def slot_positions(flat_ids, expert_count):
    entries = flat_ids.shape[1]
    onehot = (flat_ids[:, :, None] == jnp.arange(expert_count, dtype=jnp.int32)).astype(BF16)
    lower = jnp.tril(jnp.ones((entries, entries), BF16))
    running = jnp.einsum("ij,bje->bie", lower, onehot, preferred_element_type=F32)
    return jnp.sum(onehot.astype(F32) * running, axis=2).astype(jnp.int32) - 1


def ssm_part(ssm_in, b_proj, c_proj, step_sizes, a_log, skip_gain, ssm_grad):
    length, columns = ssm_in.shape
    heads = columns // HDIM
    state = b_proj.shape[1]
    blocks = length // SPAN
    parts = lax.axis_size("seq")
    me = lax.axis_index("seq")
    x = ssm_in.reshape(blocks, SPAN, heads, HDIM).transpose(2, 0, 1, 3)
    g = ssm_grad.reshape(blocks, SPAN, heads, HDIM).transpose(2, 0, 1, 3)
    b = b_proj.reshape(blocks, SPAN, state)
    c = c_proj.reshape(blocks, SPAN, state)
    rates = jnp.exp(a_log)
    q = (step_sizes * rates[:, None]).reshape(heads, blocks, SPAN)
    upper = jnp.triu(jnp.ones((SPAN, SPAN), F32))
    cum = jnp.einsum("hkj,ji->hki", q, upper, precision=PRECISE)
    total = cum[:, :, -1]
    head_decay = jnp.exp(-cum)
    tail_decay = jnp.exp(cum - total[:, :, None])
    block_decay = jnp.exp(-total)
    fresh = mm("hkjp,kjn->hkpn", tail_decay[..., None] * x.astype(F32), b)
    back = mm("hkjp,kjn->hkpn", head_decay[..., None] * g.astype(F32), c)
    end_state = fresh[:, 0]
    for k in range(1, blocks):
        end_state = block_decay[:, k, None, None] * end_state + fresh[:, k]
    entry_grad = back[:, blocks - 1]
    for k in range(blocks - 2, -1, -1):
        entry_grad = block_decay[:, k, None, None] * entry_grad + back[:, k]
    shard_decay = jnp.exp(-jnp.sum(total, axis=1))
    packed = jnp.concatenate(
        [
            end_state,
            entry_grad,
            jnp.broadcast_to(shard_decay[:, None, None], (heads, 16, state)),
        ],
        axis=1,
    ).astype(BF16)
    everyone = lax.all_gather(packed, "seq", axis=0).astype(F32)

    lower_mask = jnp.tril(jnp.ones((SPAN, SPAN), jnp.bool_))
    spread = cum[:, :, :, None] - cum[:, :, None, :]
    weights = jnp.where(lower_mask, jnp.exp(-jnp.where(lower_mask, spread, 0.0)), 0.0)
    scores = mm("kin,kjn->kij", c, b)
    pair = mm("hkip,hkjp->hkij", g, x)
    mixed = weights * scores[None]
    cross = weights * pair
    products = mixed * pair
    row_sum = jnp.sum(products, axis=3)
    column_sum = jnp.sum(products, axis=2)
    x_within = mm("hkij,hkip->hkjp", mixed, g)
    cross_sum = jnp.sum(cross, axis=0)
    b_within = mm("kij,kin->kjn", cross_sum, c)
    c_within = mm("kij,kjn->kin", cross_sum, b)

    entry = jnp.zeros((heads, HDIM, state), F32)
    leave = jnp.zeros((heads, HDIM, state), F32)
    for i in range(parts - 1):
        decay = everyone[i][:, 2 * HDIM : 2 * HDIM + 1, :]
        entry = jnp.where(i < me, decay * entry + everyone[i][:, :HDIM], entry)
    for i in range(parts - 1, 0, -1):
        decay = everyone[i][:, 2 * HDIM : 2 * HDIM + 1, :]
        leave = jnp.where(i > me, decay * leave + everyone[i][:, HDIM : 2 * HDIM], leave)
    entries = [entry]
    for k in range(blocks - 1):
        entries.append(block_decay[:, k, None, None] * entries[-1] + fresh[:, k])
    leaves = [leave]
    for k in range(blocks - 1, 0, -1):
        leaves.append(block_decay[:, k, None, None] * leaves[-1] + back[:, k])
    entries = jnp.stack(entries, axis=1)
    leaves = jnp.stack(leaves[::-1], axis=1)

    from_leave = tail_decay[..., None] * mm("kjn,hkpn->hkjp", b, leaves)
    from_entry = head_decay[..., None] * mm("kin,hkpn->hkip", c, entries)
    x_grad = x_within + from_leave + skip_gain[:, None, None, None] * g.astype(F32)
    x_grad = x_grad.transpose(1, 2, 0, 3).reshape(length, columns).astype(BF16)
    b_grad = b_within + mm("hkjp,hkpn->kjn", tail_decay[..., None] * x.astype(F32), leaves)
    c_grad = c_within + mm("hkip,hkpn->kin", head_decay[..., None] * g.astype(F32), entries)
    carried = jnp.sum(g.astype(F32) * from_entry, axis=3)
    leaving = jnp.sum(x.astype(F32) * from_leave, axis=3)
    through = block_decay * jnp.sum(leaves * entries, axis=(2, 3))
    after = jnp.einsum("hki,ij->hkj", row_sum - column_sum + carried, jnp.tril(jnp.ones((SPAN, SPAN), F32)), precision=PRECISE)
    before = jnp.einsum("hkj,ji->hki", leaving, jnp.triu(jnp.ones((SPAN, SPAN), F32), 1), precision=PRECISE)
    decay_grad = -(after + before + through[:, :, None])
    step_grads = decay_grad.reshape(heads, length) * rates[:, None]
    return (x_grad, b_grad.reshape(length, state), c_grad.reshape(length, state), step_grads)


MESH_IDS = pl.DeviceIdType.MESH
TRANSPOSED = (((1,), (1,)), ((), ()))


def col_tile(width):
    return 256 if width % 256 == 0 else 128


def expert_kernel(
    parts,
    groups,
    x_grad,
    entries,
    weight_in,
    outgoing,
    down_in,
    saved_in,
    out,
    totals_out,
    table,
    gates,
    picked,
    rows_all,
    weight,
    residual,
    down,
    moe,
    upstream,
    saved,
    staged,
    partial,
    route,
    route_in,
    totals,
    local_sem,
    saved_sem,
    staged_sem,
    send_sem,
    recv_sem,
    table_send,
    table_recv,
    pick_send,
    pick_recv,
    residual_send,
    residual_recv,
    route_sem,
):
    slots, columns = picked.shape[1:]
    capacity = slots // groups
    tokens = entries.shape[1]
    devices = parts * groups
    depth = weight.shape[0]
    hidden = down.shape[0]
    half = slots // 2
    me = lax.axis_index("seq")
    expert = lax.axis_index("exp")
    square = parts == 4
    peers = [lax.rem(me + o, parts) for o in range(1, parts)]
    beside = me + 1 - 2 * lax.rem(me, 2)
    across = lax.rem(me + 2, parts)
    corner = parts - 1 - me

    def local(source, target, number):
        return pltpu.make_async_copy(source, target, local_sem.at[number])

    weights_in = [
        local(weight_in.at[j], weight.at[:, pl.ds(j * columns, columns)], j)
        for j in range(groups)
    ]
    down_copy = local(down_in.at[0], down, groups)
    flat = me * groups + expert
    my_columns = pl.ds(pl.multiple_of(expert * columns, columns), columns)
    my_block = pl.ds(pl.multiple_of(flat * capacity, capacity), capacity)

    def outgoing_block(part, number):
        return outgoing.at[
            pl.ds(pl.multiple_of(number * capacity, capacity), capacity),
            pl.ds(pl.multiple_of(part * depth, depth), depth),
        ]

    own_entries = pltpu.make_async_copy(entries, table.at[flat], table_recv)
    own_rows = pltpu.make_async_copy(picked.at[expert], rows_all.at[me, :, my_columns], pick_recv)
    own_residual = pltpu.make_async_copy(
        outgoing_block(me, expert), residual.at[my_block], residual_recv.at[me]
    )

    def saved_copy(k):
        return pltpu.make_async_copy(
            saved_in.at[0, pl.ds(k * slots, slots)], saved.at[k % 2], saved_sem.at[k % 2]
        )

    def staged_copy(k):
        return pltpu.make_async_copy(
            staged.at[k % 2], out.at[0, pl.ds(k * slots, slots)], staged_sem.at[k % 2]
        )

    own_entries.start()
    own_residual.start()
    for copy in weights_in:
        copy.start()
    saved_copy(0).start()
    down_copy.start()

    barrier = pltpu.get_barrier_semaphore()

    def device(other):
        return (lax.div(other, groups), lax.rem(other, groups))

    def greet(o, carry):
        other = lax.rem(flat + o, devices)
        pl.semaphore_signal(barrier, inc=1, device_id=device(other), device_id_type=MESH_IDS)
        return carry

    lax.fori_loop(1, devices, greet, 0)
    pl.semaphore_wait(barrier, devices - 1)

    def pick_copy(o):
        other = lax.rem(expert + o, groups)
        return pltpu.make_async_remote_copy(
            src_ref=picked.at[other],
            dst_ref=rows_all.at[me, :, my_columns],
            send_sem=pick_send,
            recv_sem=pick_recv,
            device_id=(me, other),
            device_id_type=MESH_IDS,
        )

    def residual_copy(o):
        other = lax.rem(flat + o, devices)
        return pltpu.make_async_remote_copy(
            src_ref=outgoing_block(*device(other)),
            dst_ref=residual.at[my_block],
            send_sem=residual_send,
            recv_sem=residual_recv.at[me],
            device_id=device(other),
            device_id_type=MESH_IDS,
        )

    def start_pick(o, carry):
        pick_copy(o).start()
        return carry

    def start_residual(o, carry):
        residual_copy(o).start()
        return carry

    def start_entries(o, carry):
        other = lax.rem(flat + o, devices)
        pltpu.make_async_remote_copy(
            src_ref=entries,
            dst_ref=table.at[flat],
            send_sem=table_send,
            recv_sem=table_recv,
            device_id=device(other),
            device_id_type=MESH_IDS,
        ).start()
        return carry

    def pick(b, carry):
        entry = table[me * groups + b]
        numbers = lax.broadcasted_iota(jnp.int32, (slots, tokens), 0).astype(F32)
        hit = jnp.zeros((slots, tokens), F32)
        for j in range(TOPK):
            hit = jnp.where(numbers == entry[j : j + 1], 1.0, hit)
        block = x_grad[pl.ds(pl.multiple_of(b * tokens, tokens), tokens), :]
        found = jnp.dot(hit.astype(BF16), block, preferred_element_type=F32).astype(BF16)
        place = pl.ds(pl.multiple_of(b * capacity, capacity), capacity)
        picked[:, place, :] = found.reshape(groups, capacity, columns)
        return carry

    def gate(block, carry):
        entry = table[block]
        numbers = lax.broadcasted_iota(jnp.int32, (capacity, tokens), 0) + expert * capacity
        numbers = numbers.astype(F32)
        value = jnp.zeros((capacity, tokens), F32)
        for j in range(TOPK):
            value = jnp.where(numbers == entry[j : j + 1], entry[TOPK + j : TOPK + j + 1], value)
        place = pl.ds(pl.multiple_of(block * capacity, capacity), capacity)
        gates[place, :] = jnp.sum(value, axis=1, keepdims=True)
        return carry

    def await_all(block, sem):
        pltpu.make_async_copy(block, block, sem).wait()

    def piece(phase, owner, number):
        span = slots if number is None else half
        first = 0 if number is None else number * half
        if phase == 0:
            return rows_all.at[owner, pl.ds(first, span)]
        start = pl.multiple_of(owner * depth, depth)
        return moe.at[phase - 1, pl.ds(first, span), pl.ds(start, depth)]

    def remote(phase, owner, number, peer, index):
        block = piece(phase, owner, number)
        return pltpu.make_async_remote_copy(
            src_ref=block,
            dst_ref=block,
            send_sem=send_sem.at[phase, index],
            recv_sem=recv_sem.at[phase, index],
            device_id=(peer, expert),
            device_id_type=MESH_IDS,
        )

    def sends(phase):
        if not square:
            return [remote(phase, me, None, peers[o], o) for o in range(parts - 1)]
        return [
            remote(phase, me, 1, beside, 1),
            remote(phase, me, 0, across, 2),
            remote(phase, me, 0, beside, 0),
            remote(phase, me, 1, across, 3),
        ]

    def forward_across(phase):
        return remote(phase, beside, 1, across, 5)

    def forward_beside(phase):
        return remote(phase, across, 0, beside, 4)

    def start(phase):
        for copy in sends(phase):
            copy.start()

    def relay(phase):
        if square:
            remote(phase, beside, 1, beside, 1).wait_recv()
            forward_across(phase).start()
            remote(phase, across, 0, across, 2).wait_recv()
            forward_beside(phase).start()

    def arrive(phase):
        if square:
            remote(phase, beside, 0, beside, 0).wait_recv()
            remote(phase, across, 1, across, 3).wait_recv()
            remote(phase, corner, 0, beside, 4).wait_recv()
            remote(phase, corner, 1, across, 5).wait_recv()
        else:
            for o in range(parts - 1):
                owner = lax.rem(me + parts - 1 - o, parts)
                remote(phase, owner, None, peers[o], o).wait_recv()

    def finish(phase):
        for copy in sends(phase):
            copy.wait_send()
        if square:
            forward_across(phase).wait_send()
            forward_beside(phase).wait_send()

    def project(k):
        tile = col_tile(depth)
        rows = rows_all.at[k]
        await_all(residual.at[pl.ds(k * slots, slots)], residual_recv.at[k])

        def step(i, carry):
            first = pl.multiple_of(i * tile, tile)
            total = lax.dot_general(
                rows[...], weight[pl.ds(first, tile), :], TRANSPOSED,
                preferred_element_type=F32,
            )
            total = total + residual[pl.ds(k * slots, slots), pl.ds(first, tile)].astype(F32)
            place = pl.multiple_of(me * depth + first, tile)
            moe[k, :, pl.ds(place, tile)] = total.astype(BF16)
            return carry

        lax.fori_loop(0, depth // tile, step, 0)

    def expand(k):
        tile = col_tile(hidden)

        def step(i, carry):
            first = pl.multiple_of(i * tile, tile)
            upstream[:, pl.ds(first, tile)] = lax.dot_general(
                moe[k], down[pl.ds(first, tile), :], TRANSPOSED,
                preferred_element_type=F32,
            )
            return carry

        lax.fori_loop(0, hidden // tile, step, 0)

    def activate(k):
        tile = 32
        lanes = 128

        def step(i, carry):
            first = pl.multiple_of(i * tile, tile)
            rows = pl.ds(first, tile)
            gate_pre = saved[k % 2, rows, 0, :].astype(F32)
            up_pre = saved[k % 2, rows, 1, :].astype(F32)
            up = upstream[rows, :]
            sigmoid_gate = 1.0 / (1.0 + jnp.exp(-gate_pre))
            activated = gate_pre * sigmoid_gate
            product = activated * up_pre * up
            total = product[:, :lanes]
            for j in range(1, hidden // lanes):
                total = total + product[:, j * lanes : (j + 1) * lanes]
            partial[rows, :] = total
            scale = gates[pl.ds(pl.multiple_of(k * slots + first, tile), tile), :]
            hidden_grad = scale * up
            gate_grad = hidden_grad * up_pre * sigmoid_gate * (1.0 + gate_pre * (1.0 - sigmoid_gate))
            staged[k % 2, rows, 0, :] = gate_grad.astype(BF16)
            staged[k % 2, rows, 1, :] = (hidden_grad * activated).astype(BF16)
            return carry

        lax.fori_loop(0, slots // tile, step, 0)
        sums = jnp.sum(partial[...].T, axis=0, keepdims=True)
        route[k] = sums

        @pl.when(me == k)
        def _():
            route_in[k] = sums

        @pl.when(me != k)
        def _():
            route_copy(k).start()

    def route_copy(k):
        return pltpu.make_async_remote_copy(
            src_ref=route.at[k],
            dst_ref=route_in.at[me],
            send_sem=route_sem.at[0],
            recv_sem=route_sem.at[1],
            device_id=(k, expert),
            device_id_type=MESH_IDS,
        )

    def total_copy(o):
        return pltpu.make_async_remote_copy(
            src_ref=totals.at[expert],
            dst_ref=totals.at[expert],
            send_sem=route_sem.at[2],
            recv_sem=route_sem.at[3],
            device_id=(me, lax.rem(expert + o, groups)),
            device_id_type=MESH_IDS,
        )

    def send_totals():
        await_all(route_in.at[pl.ds(0, parts - 1)], route_sem.at[1])
        total = route_in[0]
        for k in range(1, parts):
            total = total + route_in[k]
        totals[expert] = total
        for o in range(1, groups):
            total_copy(o).start()

    def receive_totals():
        await_all(totals.at[pl.ds(0, groups - 1)], route_sem.at[3])
        totals_out[...] = totals[...]
        await_all(route.at[pl.ds(0, parts - 1)], route_sem.at[0])
        await_all(totals.at[pl.ds(0, groups - 1)], route_sem.at[2])

    lax.fori_loop(1, devices, start_entries, 0)
    first_batch = 1 + devices // 6
    lax.fori_loop(1, first_batch, start_residual, 0)
    await_all(table, table_recv)
    lax.fori_loop(0, groups, pick, 0, unroll=True)
    own_rows.start()
    lax.fori_loop(1, groups, start_pick, 0)
    lax.fori_loop(first_batch, devices, start_residual, 0)
    lax.fori_loop(0, devices, gate, 0)
    await_all(rows_all.at[me], pick_recv)
    start(0)
    for copy in weights_in:
        copy.wait()
    relay(0)
    arrive(0)
    project(0)
    start(1)
    if parts > 1:
        project(1)
    relay(1)
    start(2)
    project(2)
    down_copy.wait()
    for k in range(parts):
        arrive(k + 1)
        if k + 1 < parts:
            saved_copy(k + 1).start()
        expand(k)
        if k + 1 < parts:
            relay(k + 2)
            if k + 2 < parts:
                start(k + 3)
                if k + 3 < parts:
                    project(k + 3)
        saved_copy(k).wait()
        if k >= 2:
            staged_copy(k - 2).wait()
        activate(k)
        staged_copy(k).start()
    send_totals()
    await_all(table.at[pl.ds(0, devices - 1)], table_send)
    await_all(picked.at[pl.ds(0, groups - 1)], pick_send)
    await_all(residual.at[pl.ds(0, (devices - 1) * capacity)], residual_send)
    for phase in range(parts + 1):
        finish(phase)
    receive_totals()
    for k in range(max(0, parts - 2), parts):
        staged_copy(k).wait()


def expert_part(x_grad, entries, weight, outgoing, w_down, saved_pre):
    groups = lax.axis_size("exp")
    parts = lax.axis_size("seq")
    slots = outgoing.shape[0]
    columns = x_grad.shape[1]
    depth = weight.shape[1]
    hidden = w_down.shape[1]
    width = w_down.shape[2]
    anywhere = pl.BlockSpec(memory_space=pl.ANY)
    in_vmem = pl.BlockSpec(memory_space=pltpu.VMEM)
    copies = 6 if parts == 4 else parts - 1
    return pl.pallas_call(
        functools.partial(expert_kernel, parts, groups),
        out_shape=(
            jax.ShapeDtypeStruct(saved_pre.shape, BF16),
            jax.ShapeDtypeStruct((groups, 1, slots), F32),
        ),
        in_specs=[in_vmem] * 2 + [anywhere] * 4,
        out_specs=(anywhere, in_vmem),
        scratch_shapes=[
            pltpu.VMEM((parts * groups, *entries.shape), F32),
            pltpu.VMEM((parts * slots, 1), F32),
            pltpu.VMEM((groups, slots, columns), BF16),
            pltpu.VMEM((parts, slots, groups * columns), BF16),
            pltpu.VMEM((depth, groups * columns), BF16),
            pltpu.VMEM((parts * slots, depth), BF16),
            pltpu.VMEM((hidden, width), BF16),
            pltpu.VMEM((parts, slots, width), BF16),
            pltpu.VMEM((slots, hidden), F32),
            pltpu.VMEM((2, slots, 2, hidden), BF16),
            pltpu.VMEM((2, slots, 2, hidden), BF16),
            pltpu.VMEM((slots, 128), F32),
            pltpu.VMEM((parts, 1, slots), F32),
            pltpu.VMEM((parts, 1, slots), F32),
            pltpu.VMEM((groups, 1, slots), F32),
            pltpu.SemaphoreType.DMA((groups + 1,)),
            pltpu.SemaphoreType.DMA((2,)),
            pltpu.SemaphoreType.DMA((2,)),
            pltpu.SemaphoreType.DMA((parts + 1, copies)),
            pltpu.SemaphoreType.DMA((parts + 1, copies)),
            pltpu.SemaphoreType.DMA,
            pltpu.SemaphoreType.DMA,
            pltpu.SemaphoreType.DMA,
            pltpu.SemaphoreType.DMA,
            pltpu.SemaphoreType.DMA,
            pltpu.SemaphoreType.DMA((parts,)),
            pltpu.SemaphoreType.DMA((4,)),
        ],
        compiler_params=pltpu.CompilerParams(
            collective_id=1, has_side_effects=True, vmem_limit_bytes=62 * 1024 * 1024
        ),
        cost_estimate=pl.CostEstimate(
            flops=2 * parts * slots * (width * hidden + groups * columns * depth),
            bytes_accessed=2 * (hidden * width + 4 * parts * slots * hidden),
            transcendentals=0,
        ),
    )(x_grad, entries, weight, outgoing, w_down, saved_pre)


def per_device(
    gates,
    expert_ids,
    saved_pre,
    w_down,
    residual_grad,
    in_weight,
    ssm_in,
    b_proj,
    c_proj,
    step_sizes,
    a_log,
    skip_gain,
    ssm_grad,
):
    expert_count = lax.axis_size("exp")
    parts = lax.axis_size("seq")
    my_expert = lax.axis_index("exp")
    tokens_here, width = residual_grad.shape
    per_block = tokens_here * TOPK
    capacity = per_block // expert_count
    slots = expert_count * capacity

    entry_ids = expert_ids.reshape(1, per_block)
    own_target = (entry_ids * capacity + slot_positions(entry_ids, expert_count)).reshape(
        tokens_here, TOPK
    )
    slot_numbers = jnp.arange(slots, dtype=jnp.int32)
    own_selector = jnp.any(own_target[None] == slot_numbers[:, None, None], axis=2).astype(BF16)
    outgoing = jnp.dot(own_selector, residual_grad, preferred_element_type=F32).astype(BF16)
    slice_weight = lax.all_gather(in_weight, "exp", axis=0)
    entries = jnp.concatenate([own_target.astype(F32).T, gates.T], axis=0)
    entries = jnp.pad(entries, ((0, -entries.shape[0] % 8), (0, 0)))
    x_grad, b_grad, c_grad, step_grads = ssm_part(
        ssm_in, b_proj, c_proj, step_sizes, a_log, skip_gain, ssm_grad
    )

    both = jnp.concatenate([b_grad, c_grad], axis=1)
    both, slice_weight = lax.optimization_barrier((both, slice_weight))
    pre_grad, totals = expert_part(
        x_grad, entries, slice_weight, outgoing, w_down, saved_pre
    )
    both = lax.psum_scatter(both, "exp", scatter_dimension=0, tiled=True)
    state = b_proj.shape[1]

    totals = lax.dynamic_slice_in_dim(totals[:, 0, :], my_expert * capacity, capacity, 1)
    totals = totals.reshape(-1)
    chosen = own_target.reshape(per_block, 1) == slot_numbers[None, :]
    route_grads = jnp.sum(jnp.where(chosen, totals[None, :], 0.0), axis=1)
    return (
        pre_grad,
        route_grads.reshape(tokens_here, TOPK),
        both[:, :state],
        both[:, state:],
        step_grads,
    )


def solution(mesh):
    in_specs = (
        P(("seq", "exp"), None),
        P(("seq", "exp"), None),
        P("exp", None, None, "seq"),
        P("exp", "seq", None),
        P(("seq", "exp"), None),
        P("seq", "exp"),
        P("seq", "exp"),
        P("seq", None),
        P("seq", None),
        P("exp", "seq"),
        P("exp"),
        P("exp"),
        P("seq", "exp"),
    )
    out_specs = (
        P("exp", None, None, "seq"),
        P(("seq", "exp"), None),
        P(("seq", "exp"), None),
        P(("seq", "exp"), None),
        P("exp", "seq"),
    )
    return jax.shard_map(
        per_device, mesh=mesh, in_specs=in_specs, out_specs=out_specs, check_vma=False
    )
```
